256 devices in a mesh: img: 64 (over z, y, core), rep: 4 (over x).
Axes of the slice: x: 4, y: 4, z: 8, core: 2. Of those that a mesh axis runs over, the one named last changes fastest.
Arguments:
- descriptors: bfloat16 [128, 256, 1024], P('img', 'rep'), may hold values from -0.5 to 0.5
- cell_counts: int32 [128, 256], P('img', 'rep'), may hold values from 1 to 8
- pair_images: int32 [4096, 2], P('img'), may hold values from 0 to 127, as said below
- query_cells: int32 [4096, 16], P('img'), may hold values from 0 to 255
- cand_cells: int32 [4096, 4, 16], P('img', 'rep'), may hold values from 0 to 255, as said below
- cand_counts: int32 [4096, 4], P('img', 'rep'), may hold values from 8 to 16, as said below
Outputs:
- matches: float32 [4096, 2, 128], P('img')
- image_score: float32 [128], P('img')
The draws below stay inside these ranges and needn't reach their ends.
Inputs may be any that keep to these rules, and one draw needn't show every extreme that they name: `pair_images`: the pairs are numbered by blocks of 64: pair k * 64 + j has its first image among images k * 2 to k * 2 + 1 and its second among images j * 2 to j * 2 + 1; the two images of a pair differ. cand_cells[p, r, s] lies in quarter r, between r * 64 and r * 64 + 63; cells may repeat. `cand_counts`: every count is 8 or 16, and every draw holds at least one count of 16.
All inputs are finite; a program needn't handle non-finite values.
Results may differ from the reference program's by a relative error of at most 0.0003.
Values may be sent and summed in bfloat16 or wider, within the bound.
No kernel may reach another device: no remote copies, remote signals or barrier semaphores. Data moves between devices by JAX's collectives and lax.ppermute only.
A program may use at most 64 MiB of HBM per device.

```python
import jax
import jax.numpy as jnp
from jax import lax

DESC = 128
KP = 8
CELLS = 256
IMG_DEV = 2
QCELL = 16
SLOT = 16
QDESC = 128
IMAGES = 128
PAIRS = 4096
N_IMG = 64
N_REP = 4


def draw_pair_images(key, part):
    index = jnp.arange(N_IMG * N_IMG, dtype=jnp.int32)
    owner = index // N_IMG
    partner = index % N_IMG
    key_first = jax.random.fold_in(key, 11)
    key_second = jax.random.fold_in(key, 12)
    key_same = jax.random.fold_in(key, 13)
    local_first = jax.random.randint(key_first, (N_IMG * N_IMG,), 0, IMG_DEV, dtype=jnp.int32)
    local_any = jax.random.randint(key_second, (N_IMG * N_IMG,), 0, IMG_DEV, dtype=jnp.int32)
    local_other = jax.random.randint(key_same, (N_IMG * N_IMG,), 0, IMG_DEV - 1, dtype=jnp.int32)
    local_other = jnp.where(local_other >= local_first, local_other + 1, local_other)
    local_second = jnp.where(owner == partner, local_other, local_any)
    first = owner * IMG_DEV + local_first
    second = partner * IMG_DEV + local_second
    return jnp.stack([first, second], axis=1).astype(jnp.int32)


def draw_cand_cells(key, part):
    share = CELLS // N_REP
    offsets = jax.random.randint(jax.random.fold_in(key, 21), (N_IMG * N_IMG, N_REP, SLOT), 0, share, dtype=jnp.int32)
    quarter = jnp.arange(N_REP, dtype=jnp.int32)[None, :, None] * share
    return (offsets + quarter).astype(jnp.int32)


def draw_cand_counts(key, part):
    divisor = jax.random.randint(jax.random.fold_in(key, 31), (N_IMG * N_IMG * N_REP,), 1, 3, dtype=jnp.int32)
    counts = SLOT // divisor
    spot = jax.random.randint(jax.random.fold_in(key, 32), (), 0, N_IMG * N_IMG * N_REP, dtype=jnp.int32)
    counts = jnp.where(jnp.arange(N_IMG * N_IMG * N_REP, dtype=jnp.int32) == spot, SLOT, counts)
    return counts.reshape(N_IMG * N_IMG, N_REP).astype(jnp.int32)


def touch_ends(array, own_key, smallest, largest):
    spot = [jax.random.randint(jax.random.fold_in(own_key, axis), (), 0, length) for axis, length in enumerate(array.shape)]
    longest = array.shape.index(max(array.shape))
    next_to = spot[:longest] + [(spot[longest] + 1) % array.shape[longest]] + spot[longest + 1:]
    return array.at[tuple(spot)].set(smallest).at[tuple(next_to)].set(largest)


def levels(own_key, dims, shards, low, largest):
    gain, own = 1.0, jax.random.fold_in(own_key, 6)
    for position, blocks in shards:
        heights = jnp.exp(jax.random.uniform(jax.random.fold_in(own, position), (blocks,), jnp.float32, low / len(shards), largest / len(shards)))
        gain = gain * jnp.repeat(heights, dims[position] // blocks).reshape([-1 if axis == position else 1 for axis in range(len(dims))])
    return gain


def gaussian(rng, shape, width, limit, split=(), kind=jnp.bfloat16):
    entries = width * jax.random.normal(rng, shape, jnp.float32)
    if split:
        entries = entries * levels(rng, shape, split, -0.22, 0.18)
    return jnp.clip(entries, -limit, limit).astype(kind)


def setup_inputs(seed: int = 0) -> dict:
    keys = jax.random.split(jax.random.key(seed), 7)
    descriptors = gaussian(keys[0], (IMAGES, CELLS, KP * DESC), 0.0884, 0.5, ((0, 64), (1, 4)))
    cell_counts = touch_ends(jax.random.randint(keys[1], (IMAGES, CELLS), 1, KP + 1), jax.random.fold_in(keys[1], 1), 1, KP).astype(jnp.int32)
    pair_images = draw_pair_images(jax.random.fold_in(keys[6], 71), 0)
    query_cells = touch_ends(jax.random.randint(keys[3], (PAIRS, QCELL), 0, CELLS), jax.random.fold_in(keys[3], 1), 0, CELLS - 1).astype(jnp.int32)
    cand_cells = draw_cand_cells(jax.random.fold_in(keys[6], 71), 0)
    cand_counts = draw_cand_counts(jax.random.fold_in(keys[6], 71), 0)
    return {"descriptors": descriptors, "cell_counts": cell_counts, "pair_images": pair_images, "query_cells": query_cells, "cand_cells": cand_cells, "cand_counts": cand_counts}


distant = 1.0e9


def reference(descriptors, cell_counts, pair_images, query_cells, cand_cells, cand_counts):
    flat = descriptors.reshape(IMAGES * CELLS, KP * DESC)
    flat_counts = cell_counts.reshape(IMAGES * CELLS)
    first = pair_images[:, 0].astype(jnp.int32)
    second = pair_images[:, 1].astype(jnp.int32)
    query_rows = (first[:, None] * CELLS + query_cells).astype(jnp.int32)
    cand_rows = (second[:, None, None] * CELLS + cand_cells).astype(jnp.int32)
    slot_ids = jnp.arange(KP, dtype=jnp.int32)
    cand_ids = jnp.arange(SLOT, dtype=jnp.int32)

    def one_pair(index):
        qrow = query_rows[index]
        crow = cand_rows[index].reshape(N_REP * SLOT)
        queries = flat[qrow].reshape(QDESC, DESC).astype(jnp.float32)
        qlive = (slot_ids[None, :] < flat_counts[qrow][:, None]).reshape(QDESC)
        cands = flat[crow].reshape(N_REP * SLOT * KP, DESC).astype(jnp.float32)
        cell_live = cand_ids[None, :] < cand_counts[index][:, None]
        slot_live = slot_ids[None, None, :] < flat_counts[crow].reshape(N_REP, SLOT)[:, :, None]
        clive = (cell_live[:, :, None] & slot_live).reshape(N_REP * SLOT * KP)
        qnorm = jnp.sum(queries * queries, axis=1)
        cnorm = jnp.sum(cands * cands, axis=1)
        inner = jnp.dot(queries, cands.T, precision=lax.Precision.HIGHEST, preferred_element_type=jnp.float32)
        dist = qnorm[:, None] + cnorm[None, :] - 2.0 * inner
        dist = jnp.where(clive[None, :], dist, jnp.float32(distant))
        lowest = -lax.top_k(-dist, 2)[0]
        best = jnp.where(qlive, lowest[:, 0], jnp.float32(0.0))
        runner = jnp.where(qlive, lowest[:, 1], jnp.float32(0.0))
        margin = jnp.where(qlive, (runner - best) / (runner + 1.0), jnp.float32(0.0))
        score = jnp.sum(margin) / jnp.sum(qlive.astype(jnp.float32))
        return jnp.stack([best, runner]), score

    matches, scores = lax.map(one_pair, jnp.arange(PAIRS, dtype=jnp.int32))
    image_score = jnp.zeros((IMAGES,), jnp.float32).at[first].add(scores).at[second].add(scores)
    return matches, image_score
```

```python
import functools

import jax
import jax.numpy as jnp
from jax import lax
from jax.experimental import pallas as pl
from jax.experimental.pallas import tpu as pltpu
from jax.sharding import PartitionSpec as P

DESC = 128
KP = 8

dead_entry = 16384.0
cut = 1.0e6
f32 = jnp.float32
bf16 = jnp.bfloat16


def vmem():
    return pl.BlockSpec(memory_space=pltpu.VMEM)


def smem():
    return pl.BlockSpec(memory_space=pltpu.SMEM)


def pick_queries(rep, cells, cells_ref, first_ref, at_ref, own, one, two, three, out):
    me = at_ref[1]
    pairs = first_ref.shape[0]
    share = own.shape[0] // 2
    part = out.shape[1]

    def step(p, _):
        base = (first_ref[p, 0] & 1) * share
        for u in range(part):
            cell = cells_ref[p, me * part + u]
            row = base + cell % share
            back = (me - cell // share + rep) % rep
            tile = jnp.where(
                back < 2,
                jnp.where(back == 0, own[row], one[row]),
                jnp.where(back == 2, two[row], three[row]),
            )
            out[p, u] = tile
        return 0

    lax.fori_loop(0, pairs, step, 0)


def gather_candidates(rep, at_ref, meta, own, one, two, three, out, norms, table, cnorm):
    me = at_ref[1]
    count = own.shape[0]
    width = count + 1
    group = 4
    block = 16
    for back, source in enumerate((own, one, two, three)):
        base = ((me - back + rep) % rep) * width

        def fill(c, _, source=source, base=base):
            x = source[pl.ds(c * block, block)].astype(f32)
            table[pl.ds(base + c * block, block)] = x
            sums = jnp.sum(x * x, axis=2, keepdims=True)
            cnorm[pl.ds(base + c * block, block)] = jnp.broadcast_to(sums, x.shape)
            return 0

        lax.fori_loop(0, count // block, fill, 0)
        table[base + count] = jnp.full((KP, DESC), dead_entry, f32)
        cnorm[base + count] = jnp.full((KP, DESC), dead_entry * dead_entry * DESC, f32)

    slots = norms.shape[1] // KP // rep
    lane_group = lax.broadcasted_iota(jnp.int32, (KP, DESC), 1) // (DESC // group)

    def quad(g, _):
        for q in range(rep):
            for s in range(0, slots, 2):
                t = q * slots + s
                where = [
                    [meta[(g * group + i) * rep + q, s + h] for h in range(2)] for i in range(group)
                ]
                for i in range(group):
                    both = jnp.concatenate([table[where[i][0]], table[where[i][1]]], axis=0)
                    out[g, t * KP : (t + 2) * KP, i * DESC : (i + 1) * DESC] = both.astype(bf16)
                for h in range(2):
                    low = jnp.where(lane_group == 0, cnorm[where[0][h]], cnorm[where[1][h]])
                    high = jnp.where(lane_group == 2, cnorm[where[2][h]], cnorm[where[3][h]])
                    norms[g, (t + h) * KP : (t + h + 1) * KP, :] = jnp.where(
                        lane_group < 2, low, high
                    )
        return 0

    lax.fori_loop(0, out.shape[0], quad, 0)


def keep_two(left, right):
    low = jnp.minimum(left[0], right[0])
    high = jnp.minimum(jnp.maximum(left[0], right[0]), jnp.minimum(left[1], right[1]))
    return low, high


def match(rep, at_ref, meta, queries, cands, norms, out):
    group = 4
    size = DESC // group
    rows = cands.shape[1]
    row_ids = lax.broadcasted_iota(jnp.int32, (DESC, DESC), 0)
    lane_ids = lax.broadcasted_iota(jnp.int32, (DESC, DESC), 1)
    diagonal = row_ids == lane_ids
    lanes = lax.broadcasted_iota(jnp.int32, (KP, DESC), 1)
    lane_group = lanes // size

    def quad(g, sums):
        q = queries[pl.ds(g * group, group)].astype(f32).reshape(DESC, DESC)
        square = jnp.sum(q * q, axis=1, keepdims=True)
        spread = jnp.where(diagonal, square, 0.0).reshape(DESC // KP, KP, DESC)
        qnorm = jnp.sum(jnp.sum(spread, axis=0), axis=0, keepdims=True)
        qnorm = jnp.broadcast_to(qnorm, (KP, DESC))
        twice = q * -2.0
        right = jnp.concatenate(
            [
                jnp.where(row_ids // size == i, twice, 0.0).astype(bf16)
                for i in range(group)
            ],
            axis=1,
        )
        inner = lax.dot_general(
            cands[g], right, (((1,), (1,)), ((), ())), preferred_element_type=f32
        )
        dist = (inner + norms[g]).reshape(rows // KP, KP, DESC)
        sides = [(dist[k], dist[k + 1]) for k in range(0, rows // KP, 2)]
        sides = [(jnp.minimum(a, b), jnp.maximum(a, b)) for a, b in sides]
        while len(sides) > 1:
            sides = [keep_two(sides[k], sides[k + 1]) for k in range(0, len(sides), 2)]
        low, high = sides[0]
        for turn in (4, 2, 1):
            low, high = keep_two(
                (low, high), (pltpu.roll(low, turn, 0), pltpu.roll(high, turn, 0))
            )
        live = qnorm < cut
        best = jnp.where(live, low + qnorm, 0.0)
        runner = jnp.where(live, high + qnorm, 0.0)
        margin = (runner - best) / (runner + 1.0)
        totals, seconds = [], []
        for i in range(group):
            row = (g * group + i) * rep
            total = meta[row, 16]
            for r in range(1, rep):
                total = total + meta[row + r, 16]
            totals.append(total.astype(f32))
            seconds.append(meta[row, 17])

        def per_group(values):
            return jnp.where(
                lane_group < 2,
                jnp.where(lane_group == 0, values[0], values[1]),
                jnp.where(lane_group == 2, values[2], values[3]),
            )

        share = margin / per_group(totals)
        second = per_group(seconds)
        for i in range(group):
            left = best if i == 0 else pltpu.roll(best, DESC - size * i, 1)
            at = (size - size * i) % DESC
            other = runner if at == 0 else pltpu.roll(runner, at, 1)
            line = jnp.where(
                lanes < size, left, jnp.where(lanes < 2 * size, other, totals[i])
            )
            out[g * group + i] = line[:rep]
        return (
            sums[0] + jnp.where(second == 0, share, 0.0),
            sums[1] + jnp.where(second == 0, 0.0, share),
        )

    zero = jnp.zeros((KP, DESC), f32)
    sums = lax.fori_loop(0, cands.shape[0], quad, (zero, zero))
    here = at_ref[0]
    parts = [jnp.sum(part[:1], axis=1, keepdims=True) for part in sums]
    line = out[here]
    ids = lanes[:rep]
    out[here] = jnp.where(
        ids < 3 * size, line, jnp.where(ids < 3 * size + size // 2, parts[0], parts[1])
    )


def finish(rep, at_ref, shares, first, matches, scores):
    size = DESC // rep
    here = at_ref[0]
    pairs = matches.shape[0]
    lane_group = lax.broadcasted_iota(jnp.int32, (pairs, DESC), 1) // size
    best = jnp.zeros((pairs, DESC), f32)
    runner = jnp.zeros((pairs, DESC), f32)
    for r in range(rep):
        part = shares[:, r, :]
        left = part if r == 0 else pltpu.roll(part, size * r, 1)
        at = (size * r - size) % DESC
        other = part if at == 0 else pltpu.roll(part, at, 1)
        best = jnp.where(lane_group == r, left, best)
        runner = jnp.where(lane_group == r, other, runner)
    matches[:, 0, :] = best
    matches[:, 1, :] = runner
    total = shares[:, 0, 2 * size : 2 * size + 1]
    score = jnp.sum((runner - best) / (runner + 1.0), axis=1, keepdims=True) / total
    which = first[:, :1]
    mine = shares[here]
    for b in range(2):
        own_part = jnp.sum(jnp.where(which == b, score, 0.0))
        at = 3 * size + b * (size // 2)
        scores[b] = own_part + jnp.sum(mine[:, at : at + 1])


def on_device(descriptors, cell_counts, pair_images, query_cells, cand_cells, cand_counts):
    img_dev, share, width = descriptors.shape
    peers = lax.axis_size("img")
    rep = lax.axis_size("rep")
    me = lax.axis_index("rep").astype(jnp.int32)
    at = jnp.stack([lax.axis_index("img").astype(jnp.int32), me])
    slots = cand_cells.shape[2]
    part = query_cells.shape[1] // rep
    cells = img_dev * share

    slot_ids = jnp.arange(KP, dtype=jnp.int32)
    live = slot_ids[None, :] < cell_counts.reshape(cells)[:, None]
    own = jnp.where(live[:, :, None], descriptors.reshape(cells, KP, DESC), bf16(dead_entry))

    def turned(by):
        return lax.ppermute(own, "rep", [(r, (r + by) % rep) for r in range(rep)])

    one, three, two = turned(1), turned(3), turned(2)

    first = pair_images[:, 0] % img_dev
    second = pair_images[:, 1] % img_dev
    rows = second[:, None] * share + cand_cells[:, 0, :] % share
    alive = jnp.arange(slots, dtype=jnp.int32)[None, :] < cand_counts
    rows = jnp.where(alive, rows, cells) + me * (cells + 1)
    local = first[:, None] * share + query_cells - me * share
    inside = (query_cells >= me * share) & (query_cells < (me + 1) * share)
    local = jnp.where(inside, local, -1)
    hits = local[:, :, None] == jnp.arange(cells, dtype=jnp.int32)[None, None, :]
    partial = jnp.sum(jnp.where(hits, cell_counts.reshape(cells)[None, None, :], 0), axis=(1, 2))
    note = jnp.concatenate([rows, partial[:, None], second[:, None]], axis=1)
    note = jnp.pad(note, ((0, 0), (0, DESC - note.shape[1])))
    note = jnp.broadcast_to(note[:, None, :], (peers, rep, DESC)).reshape(peers * rep, 1, DESC)
    meta = lax.all_to_all(note, ("img", "rep"), split_axis=0, concat_axis=0, tiled=True)
    meta = meta.reshape(peers * rep, DESC)

    message = pl.pallas_call(
        functools.partial(pick_queries, rep, cells),
        out_shape=jax.ShapeDtypeStruct((peers, part, KP, DESC), bf16),
        in_specs=[smem(), smem(), smem(), vmem(), vmem(), vmem(), vmem()],
        out_specs=vmem(),
        name="pick_queries",
    )(query_cells, pair_images, at, own, one, two, three)
    queries = lax.all_to_all(
        message.reshape(peers, part * KP, DESC), "img", split_axis=0, concat_axis=0, tiled=True
    )

    quads = peers // 4
    lines = rep * slots * KP
    cands, norms = pl.pallas_call(
        functools.partial(gather_candidates, rep),
        out_shape=(
            jax.ShapeDtypeStruct((quads, lines, 4 * DESC), bf16),
            jax.ShapeDtypeStruct((quads, lines, DESC), f32),
        ),
        in_specs=[smem(), smem(), vmem(), vmem(), vmem(), vmem()],
        out_specs=(vmem(), vmem()),
        scratch_shapes=[
            pltpu.VMEM((rep * (cells + 1), KP, DESC), f32),
            pltpu.VMEM((rep * (cells + 1), KP, DESC), f32),
        ],
        name="gather_candidates",
    )(at, meta, own, one, two, three)

    shares = pl.pallas_call(
        functools.partial(match, rep),
        out_shape=jax.ShapeDtypeStruct((peers, rep, DESC), f32),
        in_specs=[smem(), smem(), vmem(), vmem(), vmem()],
        out_specs=vmem(),
        name="match",
    )(at, meta, queries, cands, norms)
    shares = lax.all_to_all(
        shares.reshape(peers * rep, 1, DESC), ("img", "rep"), split_axis=0, concat_axis=0, tiled=True
    ).reshape(peers, rep, DESC)

    return pl.pallas_call(
        functools.partial(finish, rep),
        out_shape=(
            jax.ShapeDtypeStruct((peers, 2, DESC), f32),
            jax.ShapeDtypeStruct((img_dev,), f32),
        ),
        in_specs=[smem(), vmem(), vmem()],
        out_specs=(vmem(), smem()),
        name="finish",
    )(at, shares, jnp.broadcast_to(first[:, None], (peers, DESC)))


def solution(mesh):
    in_specs = (
        P("img", "rep", None),
        P("img", "rep"),
        P("img", None),
        P("img", None),
        P("img", "rep", None),
        P("img", "rep"),
    )
    out_specs = (P("img", None, None), P("img"))
    return jax.shard_map(
        on_device, mesh=mesh, in_specs=in_specs, out_specs=out_specs, check_vma=False
    )
```

```python
import functools

import jax
import jax.numpy as jnp
from jax import lax
from jax.experimental import pallas as pl
from jax.experimental.pallas import tpu as pltpu
from jax.sharding import PartitionSpec as P

DESC = 128
KP = 8
GROUP = 4
QUADS = 4

dead_entry = 16384.0
cut = 1.0e6
f32 = jnp.float32
bf16 = jnp.bfloat16
i32 = jnp.int32

at_total, at_second, at_first, at_source = 64, 65, 66, 80


def room(mib):
    return pltpu.CompilerParams(vmem_limit_bytes=mib << 20)


def vmem():
    return pl.BlockSpec(memory_space=pltpu.VMEM)


def smem():
    return pl.BlockSpec(memory_space=pltpu.SMEM)


def write_notes(rep, share, cand, query, images, live, counts, note, board):
    me = lax.axis_index("rep")
    cells = 2 * share
    pairs = cand.shape[1]
    first = images[0:1, :] & 1
    second = images[1:2, :] & 1
    slot = lax.broadcasted_iota(i32, cand.shape, 0)
    rows = jnp.where(slot < live[...], second * share + (cand[...] & (share - 1)), cells)
    cell = query[...]
    quarter = lax.shift_right_logical(cell, share.bit_length() - 1)
    local = first * share + (cell & (share - 1))
    source = ((me - quarter) & (rep - 1)) * cells + local
    local = jnp.where(quarter == me, local, -1)
    ids = lax.broadcasted_iota(i32, (cells, pairs), 0)
    hits = jnp.zeros((cells, pairs), f32)
    for t in range(local.shape[0]):
        hits = hits + jnp.where(ids == local[t : t + 1, :], 1.0, 0.0)
    total = jnp.zeros((1, pairs), f32)
    for b in range(2):
        total = total + jnp.dot(
            counts[b : b + 1, :].astype(f32),
            hits[b * share : (b + 1) * share],
            preferred_element_type=f32,
        )
    board[...] = jnp.zeros_like(board)
    slots = rows.shape[0]
    spot = pl.ds(pl.multiple_of(me * slots, slots), slots)
    board[spot, 0:pairs] = rows.astype(f32) * (2.0 * KP)
    board[at_total : at_total + 1, 0:pairs] = total
    once = jnp.where(me == 0, 1, 0)
    board[at_second : at_second + 1, 0:pairs] = (second * once).astype(f32)
    board[at_first : at_first + 1, 0:pairs] = (first * once).astype(f32)
    board[at_source : at_source + source.shape[0], 0:pairs] = source.astype(f32)
    note[...] = board[...].T[:pairs].astype(i32)


def pick_queries(rep, note, own, one, two, three, out, every):
    count = own.shape[0]
    part = out.shape[1]
    block = 32
    unroll = 8
    start = at_source + lax.axis_index("rep") * part

    def fill(c, _):
        for back, source in enumerate((own, one, two, three)):
            every[pl.ds(back * count + c * block, block)] = source[pl.ds(c * block, block)]
        return 0

    lax.fori_loop(0, count // block, fill, 0)

    def step(c, _):
        for k in range(unroll):
            for u in range(part):
                p = c * unroll + k
                out[p, u] = every[note[p, start + u]]
        return 0

    lax.fori_loop(0, out.shape[0] // unroll, step, 0)


def keep_two(left, right):
    low = jnp.minimum(left[0], right[0])
    high = jnp.minimum(jnp.maximum(left[0], right[0]), jnp.minimum(left[1], right[1]))
    return low, high


def fill_tables(every, tables):
    count = every.shape[0] // len(tables)
    block = 16
    me = lax.axis_index("rep")

    def fill(c, _):
        for quarter, table in enumerate(tables):
            back = (me - quarter) & (len(tables) - 1)
            x = every[pl.ds(back * count + c * block, block)].astype(f32)
            sums = jnp.broadcast_to(jnp.sum(x * x, axis=2, keepdims=True), x.shape)
            both = jnp.concatenate([x, sums], axis=1).reshape(block * 2 * KP, DESC)
            table[pl.ds(pl.multiple_of(c * (block * 2 * KP), 2 * KP), block * 2 * KP)] = both
        return 0

    lax.fori_loop(0, count // block, fill, 0)
    for table in tables:
        end = count * 2 * KP
        table[end : end + KP] = jnp.full((KP, DESC), dead_entry, f32)
        table[end + KP : end + 2 * KP] = jnp.full((KP, DESC), dead_entry * dead_entry * DESC, f32)


def match(rep, slots, meta, every, queries, out, *scratch):
    size = DESC // GROUP
    quads = queries.shape[0] // GROUP
    tables, norms = scratch[:rep], scratch[rep:]
    row_ids = lax.broadcasted_iota(i32, (DESC, DESC), 0)
    lane_ids = lax.broadcasted_iota(i32, (DESC, DESC), 1)
    diagonal = row_ids == lane_ids
    lanes = lax.broadcasted_iota(i32, (KP, DESC), 1)
    lane_group = lanes // size
    fill_tables(every, tables)

    def per_group(values):
        return jnp.where(
            lane_group < 2,
            jnp.where(lane_group == 0, values[0], values[1]),
            jnp.where(lane_group == 2, values[2], values[3]),
        )

    def quad(g, norms):
        q = queries[pl.ds(g * GROUP, GROUP)].astype(f32).reshape(DESC, DESC)
        square = jnp.sum(q * q, axis=1, keepdims=True)
        spread = jnp.where(diagonal, square, 0.0).reshape(DESC // KP, KP, DESC)
        qnorm = jnp.sum(jnp.sum(spread, axis=0), axis=0, keepdims=True)
        qnorm = jnp.broadcast_to(qnorm, (KP, DESC))
        twice = q * -2.0
        right = jnp.concatenate(
            [jnp.where(row_ids // size == i, twice, 0.0) for i in range(GROUP)], axis=1
        )
        columns, at = [[] for _ in range(GROUP)], 0
        for quarter, table in enumerate(tables):
            for s in range(slots):
                found = []
                for i in range(GROUP):
                    row = pl.multiple_of(meta[g * GROUP + i, quarter * slots + s], 2 * KP)
                    both = table[pl.ds(row, 2 * KP)]
                    columns[i].append(both[:KP])
                    found.append(both[KP:])
                norms[at : at + KP] = per_group(found)
                at += KP
        left = jnp.concatenate([jnp.concatenate(part, axis=0) for part in columns], axis=1)
        inner = lax.dot_general(
            left, right, (((1,), (1,)), ((), ())), preferred_element_type=f32
        )
        dist = [inner[k : k + KP] + norms[k : k + KP] for k in range(0, at, KP)]
        sides = [(dist[k], dist[k + 1]) for k in range(0, len(dist), 2)]
        sides = [(jnp.minimum(a, b), jnp.maximum(a, b)) for a, b in sides]
        while len(sides) > 1:
            sides = [keep_two(sides[k], sides[k + 1]) for k in range(0, len(sides), 2)]
        low, high = sides[0]
        for turn in (4, 2, 1):
            low, high = keep_two(
                (low, high), (pltpu.roll(low, turn, 0), pltpu.roll(high, turn, 0))
            )
        live = qnorm < cut
        best = jnp.where(live, low + qnorm, 0.0)
        runner = jnp.where(live, high + qnorm, 0.0)
        rows = [g * GROUP + i for i in range(GROUP)]
        total = per_group([meta[p, at_total].astype(f32) for p in rows])
        second = per_group([meta[p, at_second] for p in rows]).astype(f32)
        first = per_group([meta[p, at_first] for p in rows]).astype(f32)
        share = (runner - best) / ((runner + 1.0) * total)
        for i in range(GROUP):
            left, other, count, which = (
                v if at == 0 else pltpu.roll(v, at, 1)
                for v, at in (
                    (best, (DESC - size * i) % DESC),
                    (runner, (size - size * i) % DESC),
                    (total, (2 * size - size * i) % DESC),
                    (first, (2 * size - size * i) % DESC),
                )
            )
            line = jnp.where(lanes < size, left, jnp.where(lanes < 2 * size, other, count))
            line = jnp.where(lanes < 2 * size + size // 2, line, which)
            out[g * GROUP + i] = line[:rep]
        return jnp.where(second == 0.0, share, 0.0), jnp.where(second == 0.0, 0.0, share)

    def step(c, sums):
        for h in range(QUADS):
            parts = quad(c * QUADS + h, norms[h])
            sums = tuple(a + b for a, b in zip(sums, parts))
        return sums

    zero = jnp.zeros((KP, DESC), f32)
    sums = lax.fori_loop(0, quads // QUADS, step, (zero, zero))
    here = lax.axis_index("img")
    parts = [jnp.sum(part[:1], axis=1, keepdims=True) for part in sums]
    ids = lanes[:rep]
    out[here] = jnp.where(
        ids < 3 * size,
        out[here],
        jnp.where(ids < 3 * size + size // 2, parts[0], parts[1]),
    )


def finish(rep, shares, matches, scores):
    size = DESC // rep
    here = lax.axis_index("img")
    pairs = matches.shape[0]
    lane_group = lax.broadcasted_iota(i32, (pairs, DESC), 1) // size
    best = jnp.zeros((pairs, DESC), f32)
    runner = jnp.zeros((pairs, DESC), f32)
    for r in range(rep):
        part = shares[:, r, :]
        left = part if r == 0 else pltpu.roll(part, size * r, 1)
        at = (size * r - size) % DESC
        other = part if at == 0 else pltpu.roll(part, at, 1)
        best = jnp.where(lane_group == r, left, best)
        runner = jnp.where(lane_group == r, other, runner)
    matches[:, 0, :] = best
    matches[:, 1, :] = runner
    total = shares[:, 0, 2 * size : 2 * size + 1]
    score = jnp.sum((runner - best) / (runner + 1.0), axis=1, keepdims=True) / total
    at = 2 * size + size // 2
    which = shares[:, 0, at : at + 1]
    mine = shares[here]
    for b in range(2):
        own_part = jnp.sum(jnp.where(which == float(b), score, 0.0))
        at = 3 * size + b * (size // 2)
        scores[b] = own_part + jnp.sum(mine[:, at : at + 1])


def on_device(descriptors, cell_counts, pair_images, query_cells, cand_cells, cand_counts):
    img_dev, share, width = descriptors.shape
    peers = lax.axis_size("img")
    rep = lax.axis_size("rep")
    slots = cand_cells.shape[2]
    part = query_cells.shape[1] // rep
    cells = img_dev * share

    live = lax.broadcasted_iota(i32, (img_dev, share, KP), 2) < cell_counts[:, :, None]
    own = descriptors.reshape(img_dev, share, KP, DESC)
    own = jnp.where(live[:, :, :, None], own, bf16(dead_entry)).reshape(cells, KP, DESC)

    def turned(x, by):
        return lax.ppermute(x, "rep", [(r, (r + by) % rep) for r in range(rep)])

    one, two, three = (turned(own, by) for by in range(1, rep))

    note = pl.pallas_call(
        functools.partial(write_notes, rep, share),
        out_shape=jax.ShapeDtypeStruct((peers, DESC), i32),
        in_specs=[vmem()] * 5,
        out_specs=vmem(),
        scratch_shapes=[pltpu.VMEM((DESC, DESC), f32)],
        name="write_notes",
    )(cand_cells[:, 0, :].T, query_cells.T, pair_images.T, cand_counts.T, cell_counts)
    meta = lax.all_to_all(
        note.reshape(peers, 1, DESC), "img", split_axis=0, concat_axis=0, tiled=True
    ).reshape(peers, DESC)

    message, every = pl.pallas_call(
        functools.partial(pick_queries, rep),
        out_shape=(
            jax.ShapeDtypeStruct((peers, part, KP, DESC), bf16),
            jax.ShapeDtypeStruct((rep * cells, KP, DESC), bf16),
        ),
        in_specs=[smem()] + [vmem()] * 4,
        out_specs=(vmem(), vmem()),
        compiler_params=room(2),
        name="pick_queries",
    )(note, own, one, two, three)
    queries = lax.all_to_all(
        message.reshape(peers, part * KP, DESC), "img", split_axis=0, concat_axis=0, tiled=True
    )
    meta = sum((turned(meta, by) for by in range(1, rep)), meta)

    shares = pl.pallas_call(
        functools.partial(match, rep, slots),
        out_shape=jax.ShapeDtypeStruct((peers, rep, DESC), f32),
        in_specs=[smem(), vmem(), vmem()],
        out_specs=vmem(),
        scratch_shapes=[pltpu.VMEM(((cells + 1) * 2 * KP, DESC), f32)] * rep
        + [pltpu.VMEM((rep * slots * KP, DESC), f32)] * QUADS,
        compiler_params=pltpu.CompilerParams(vmem_limit_bytes=8<<20),
        name="match",
    )(meta, every, queries)
    shares = lax.all_to_all(
        shares.reshape(peers * rep, 1, DESC), ("img", "rep"), split_axis=0, concat_axis=0, tiled=True
    ).reshape(peers, rep, DESC)

    return pl.pallas_call(
        functools.partial(finish, rep),
        out_shape=(
            jax.ShapeDtypeStruct((peers, 2, DESC), f32),
            jax.ShapeDtypeStruct((img_dev,), f32),
        ),
        in_specs=[vmem()],
        out_specs=(vmem(), smem()),
        compiler_params=room(4),
        name="finish",
    )(shares)


def solution(mesh):
    in_specs = (
        P("img", "rep", None),
        P("img", "rep"),
        P("img", None),
        P("img", None),
        P("img", "rep", None),
        P("img", "rep"),
    )
    out_specs = (P("img", None, None), P("img"))
    return jax.shard_map(
        on_device, mesh=mesh, in_specs=in_specs, out_specs=out_specs, check_vma=False
    )
```

```python
import functools

import jax
import jax.numpy as jnp
from jax import lax
from jax.experimental import pallas as pl
from jax.experimental.pallas import tpu as pltpu
from jax.sharding import PartitionSpec as P

DESC = 128
KP = 8
GROUP = 4
QUADS = 8

dead_entry = 16384.0
cut = 1.0e6
f32 = jnp.float32
bf16 = jnp.bfloat16
i32 = jnp.int32

at_total, at_second, at_first, at_source = 64, 65, 66, 80


def room(mib):
    return pltpu.CompilerParams(vmem_limit_bytes=mib << 20)


def vmem():
    return pl.BlockSpec(memory_space=pltpu.VMEM)


def anywhere():
    return pl.BlockSpec(memory_space=pl.ANY)


def smem():
    return pl.BlockSpec(memory_space=pltpu.SMEM)


def write_notes(rep, share, cand, query, images, live, counts, note, board):
    me = lax.axis_index("rep")
    cells = 2 * share
    pairs = cand.shape[1]
    first = images[0:1, :] & 1
    second = images[1:2, :] & 1
    slot = lax.broadcasted_iota(i32, cand.shape, 0)
    rows = jnp.where(slot < live[...], second * share + (cand[...] & (share - 1)), cells)
    cell = query[...]
    quarter = lax.shift_right_logical(cell, share.bit_length() - 1)
    local = first * share + (cell & (share - 1))
    source = ((me - quarter) & (rep - 1)) * cells + local
    local = jnp.where(quarter == me, local, -1)
    ids = lax.broadcasted_iota(i32, (cells, pairs), 0)
    hits = jnp.zeros((cells, pairs), f32)
    for t in range(local.shape[0]):
        hits = hits + jnp.where(ids == local[t : t + 1, :], 1.0, 0.0)
    total = jnp.zeros((1, pairs), f32)
    for b in range(2):
        total = total + jnp.dot(
            counts[b : b + 1, :].astype(f32),
            hits[b * share : (b + 1) * share],
            preferred_element_type=f32,
        )
    board[...] = jnp.zeros_like(board)
    slots = rows.shape[0]
    spot = pl.ds(pl.multiple_of(me * slots, slots), slots)
    board[spot, 0:pairs] = rows.astype(f32) * (2.0 * KP)
    board[at_total : at_total + 1, 0:pairs] = total
    once = jnp.where(me == 0, 1, 0)
    board[at_second : at_second + 1, 0:pairs] = (second * once).astype(f32)
    board[at_first : at_first + 1, 0:pairs] = (first * once).astype(f32)
    board[at_source : at_source + source.shape[0], 0:pairs] = source.astype(f32)
    note[...] = board[...].T[:pairs].astype(i32)


def pick_queries(rep, note_ref, own, one, two, three, out_ref, every, note, out, sems):
    count = own.shape[0]
    part = out.shape[1]
    block = 32
    unroll = 16
    steps = out.shape[0] // unroll
    start = at_source + lax.axis_index("rep") * part
    load = pltpu.make_async_copy(note_ref, note, sems.at[steps])
    load.start()

    def fill(c, _):
        for back, source in enumerate((own, one, two, three)):
            every[pl.ds(back * count + c * block, block)] = source[pl.ds(c * block, block)]
        return 0

    lax.fori_loop(0, count // block, fill, 0)
    load.wait()

    def store(c):
        at = pl.ds(c * unroll, unroll)
        return pltpu.make_async_copy(out.at[at], out_ref.at[at], sems.at[c])

    def step(c, _):
        for k in range(unroll):
            for u in range(part):
                p = c * unroll + k
                out[p, u] = every[note[p, start + u]]

        @pl.when(c > 0)
        def _():
            store(c - 1).start()

        return 0

    lax.fori_loop(0, steps, step, 0)
    store(steps - 1).start()
    for c in range(steps):
        store(c).wait()


def keep_two(left, right):
    low = jnp.minimum(left[0], right[0])
    high = jnp.minimum(jnp.maximum(left[0], right[0]), jnp.minimum(left[1], right[1]))
    return low, high


def fill_tables(every, tables):
    count = every.shape[0] // len(tables)
    block = 16
    me = lax.axis_index("rep")

    def fill(c, _):
        for quarter, table in enumerate(tables):
            back = (me - quarter) & (len(tables) - 1)
            x = every[pl.ds(back * count + c * block, block)].astype(f32)
            sums = jnp.broadcast_to(jnp.sum(x * x, axis=2, keepdims=True), x.shape)
            both = jnp.concatenate([x, sums], axis=1).reshape(block * 2 * KP, DESC)
            table[pl.ds(pl.multiple_of(c * (block * 2 * KP), 2 * KP), block * 2 * KP)] = both
        return 0

    lax.fori_loop(0, count // block, fill, 0)
    for table in tables:
        end = count * 2 * KP
        table[end : end + KP] = jnp.full((KP, DESC), dead_entry, f32)
        table[end + KP : end + 2 * KP] = jnp.full((KP, DESC), dead_entry * dead_entry * DESC, f32)


def match(rep, slots, meta_ref, every, queries, out, meta, sem, *scratch):
    size = DESC // GROUP
    quads = queries.shape[0] // GROUP
    tables, norms = scratch[:rep], scratch[rep:]
    row_ids = lax.broadcasted_iota(i32, (DESC, DESC), 0)
    lane_ids = lax.broadcasted_iota(i32, (DESC, DESC), 1)
    diagonal = row_ids == lane_ids
    lanes = lax.broadcasted_iota(i32, (KP, DESC), 1)
    lane_group = lanes // size
    load = pltpu.make_async_copy(meta_ref, meta, sem)
    load.start()
    fill_tables(every, tables)
    load.wait()

    def per_group(values):
        return jnp.where(
            lane_group < 2,
            jnp.where(lane_group == 0, values[0], values[1]),
            jnp.where(lane_group == 2, values[2], values[3]),
        )

    def quad(g, norms):
        q = queries[pl.ds(g * GROUP, GROUP)].astype(f32).reshape(DESC, DESC)
        square = jnp.sum(q * q, axis=1, keepdims=True)
        spread = jnp.where(diagonal, square, 0.0).reshape(DESC // KP, KP, DESC)
        qnorm = jnp.sum(jnp.sum(spread, axis=0), axis=0, keepdims=True)
        qnorm = jnp.broadcast_to(qnorm, (KP, DESC))
        twice = q * -2.0
        blank = jnp.zeros((size, DESC), f32)
        right = jnp.concatenate(
            [
                jnp.concatenate(
                    [twice[i * size : (i + 1) * size] if i == j else blank for i in range(GROUP)],
                    axis=0,
                )
                for j in range(GROUP)
            ],
            axis=1,
        )
        columns, at = [[] for _ in range(GROUP)], 0
        for quarter, table in enumerate(tables):
            for s in range(slots):
                found = []
                for i in range(GROUP):
                    row = pl.multiple_of(meta[g * GROUP + i, quarter * slots + s], 2 * KP)
                    both = table[pl.ds(row, 2 * KP)]
                    columns[i].append(both[:KP])
                    found.append(both[KP:])
                norms[at : at + KP] = per_group(found)
                at += KP
        left = jnp.concatenate([jnp.concatenate(part, axis=0) for part in columns], axis=1)
        inner = lax.dot_general(
            left, right, (((1,), (1,)), ((), ())), preferred_element_type=f32
        )
        dist = [inner[k : k + KP] + norms[k : k + KP] for k in range(0, at, KP)]
        sides = [(dist[k], dist[k + 1]) for k in range(0, len(dist), 2)]
        sides = [(jnp.minimum(a, b), jnp.maximum(a, b)) for a, b in sides]
        while len(sides) > 1:
            sides = [keep_two(sides[k], sides[k + 1]) for k in range(0, len(sides), 2)]
        low, high = sides[0]
        for turn in (4, 2, 1):
            low, high = keep_two(
                (low, high), (pltpu.roll(low, turn, 0), pltpu.roll(high, turn, 0))
            )
        live = qnorm < cut
        best = jnp.where(live, low + qnorm, 0.0)
        runner = jnp.where(live, high + qnorm, 0.0)
        rows = [g * GROUP + i for i in range(GROUP)]
        total = per_group([meta[p, at_total].astype(f32) for p in rows])
        second = per_group([meta[p, at_second] for p in rows]).astype(f32)
        first = per_group([meta[p, at_first] for p in rows]).astype(f32)
        share = (runner - best) / ((runner + 1.0) * total)
        for i in range(GROUP):
            left, other, count, which = (
                v if at == 0 else pltpu.roll(v, at, 1)
                for v, at in (
                    (best, (DESC - size * i) % DESC),
                    (runner, (size - size * i) % DESC),
                    (total, (2 * size - size * i) % DESC),
                    (first, (2 * size - size * i) % DESC),
                )
            )
            line = jnp.where(lanes < size, left, jnp.where(lanes < 2 * size, other, count))
            line = jnp.where(lanes < 2 * size + size // 2, line, which)
            out[g * GROUP + i] = line[:rep]
        return jnp.where(second == 0.0, share, 0.0), jnp.where(second == 0.0, 0.0, share)

    def step(c, sums):
        for h in range(QUADS):
            parts = quad(c * QUADS + h, norms[h])
            sums = tuple(a + b for a, b in zip(sums, parts))
        return sums

    zero = jnp.zeros((KP, DESC), f32)
    sums = lax.fori_loop(0, quads // QUADS, step, (zero, zero))
    here = lax.axis_index("img")
    parts = [jnp.sum(part[:1], axis=1, keepdims=True) for part in sums]
    ids = lanes[:rep]
    out[here] = jnp.where(
        ids < 3 * size,
        out[here],
        jnp.where(ids < 3 * size + size // 2, parts[0], parts[1]),
    )


def finish(rep, shares, matches, scores):
    size = DESC // rep
    here = lax.axis_index("img")
    pairs = matches.shape[0]
    lane_group = lax.broadcasted_iota(i32, (pairs, DESC), 1) // size
    best = jnp.zeros((pairs, DESC), f32)
    runner = jnp.zeros((pairs, DESC), f32)
    for r in range(rep):
        part = shares[:, r, :]
        left = part if r == 0 else pltpu.roll(part, size * r, 1)
        at = (size * r - size) % DESC
        other = part if at == 0 else pltpu.roll(part, at, 1)
        best = jnp.where(lane_group == r, left, best)
        runner = jnp.where(lane_group == r, other, runner)
    matches[:, 0, :] = best
    matches[:, 1, :] = runner
    total = shares[:, 0, 2 * size : 2 * size + 1]
    score = jnp.sum((runner - best) / (runner + 1.0), axis=1, keepdims=True) / total
    at = 2 * size + size // 2
    which = shares[:, 0, at : at + 1]
    mine = shares[here]
    for b in range(2):
        own_part = jnp.sum(jnp.where(which == float(b), score, 0.0))
        at = 3 * size + b * (size // 2)
        scores[b] = own_part + jnp.sum(mine[:, at : at + 1])


def on_device(descriptors, cell_counts, pair_images, query_cells, cand_cells, cand_counts):
    img_dev, share, width = descriptors.shape
    peers = lax.axis_size("img")
    rep = lax.axis_size("rep")
    slots = cand_cells.shape[2]
    part = query_cells.shape[1] // rep
    cells = img_dev * share

    own = descriptors.reshape(img_dev, share, KP, DESC)
    own, counts = lax.optimization_barrier((own, cell_counts))
    live = lax.broadcasted_iota(i32, (img_dev, share, KP), 2) < counts[:, :, None]
    live = lax.optimization_barrier(live)
    own = jnp.where(live[:, :, :, None], own, bf16(dead_entry)).reshape(cells, KP, DESC)

    def turned(x, by):
        return lax.ppermute(x, "rep", [(r, (r + by) % rep) for r in range(rep)])

    one, two, three = (turned(own, by) for by in range(1, rep))

    note = pl.pallas_call(
        functools.partial(write_notes, rep, share),
        out_shape=jax.ShapeDtypeStruct((peers, DESC), i32),
        in_specs=[vmem()] * 5,
        out_specs=vmem(),
        scratch_shapes=[pltpu.VMEM((DESC, DESC), f32)],
        name="write_notes",
    )(cand_cells[:, 0, :].T, query_cells.T, pair_images.T, cand_counts.T, cell_counts)
    meta = lax.all_to_all(
        note.reshape(peers, 1, DESC), "img", split_axis=0, concat_axis=0, tiled=True
    ).reshape(peers, DESC)

    message, every = pl.pallas_call(
        functools.partial(pick_queries, rep),
        out_shape=(
            jax.ShapeDtypeStruct((peers, part, KP, DESC), bf16),
            jax.ShapeDtypeStruct((rep * cells, KP, DESC), bf16),
        ),
        in_specs=[anywhere()] + [vmem()] * 4,
        out_specs=(anywhere(), vmem()),
        scratch_shapes=[
            pltpu.SMEM((peers, DESC), i32),
            pltpu.VMEM((peers, part, KP, DESC), bf16),
            pltpu.SemaphoreType.DMA((5,)),
        ],
        compiler_params=room(2),
        name="pick_queries",
    )(note, own, one, two, three)
    queries = lax.all_to_all(
        message.reshape(peers, part * KP, DESC), "img", split_axis=0, concat_axis=0, tiled=True
    )
    meta = sum((turned(meta, by) for by in range(1, rep)), meta)

    shares = pl.pallas_call(
        functools.partial(match, rep, slots),
        out_shape=jax.ShapeDtypeStruct((peers, rep, DESC), f32),
        in_specs=[anywhere(), vmem(), vmem()],
        out_specs=vmem(),
        scratch_shapes=[pltpu.SMEM((peers, DESC), i32), pltpu.SemaphoreType.DMA]
        + [pltpu.VMEM(((cells + 1) * 2 * KP, DESC), f32)] * rep
        + [pltpu.VMEM((rep * slots * KP, DESC), f32)] * QUADS,
        compiler_params=pltpu.CompilerParams(vmem_limit_bytes=8<<20),
        name="match",
    )(meta, every, queries)
    shares = lax.all_to_all(
        shares.reshape(peers * rep, 1, DESC), ("img", "rep"), split_axis=0, concat_axis=0, tiled=True
    ).reshape(peers, rep, DESC)

    return pl.pallas_call(
        functools.partial(finish, rep),
        out_shape=(
            jax.ShapeDtypeStruct((peers, 2, DESC), f32),
            jax.ShapeDtypeStruct((img_dev,), f32),
        ),
        in_specs=[vmem()],
        out_specs=(vmem(), smem()),
        compiler_params=room(4),
        name="finish",
    )(shares)


def solution(mesh):
    in_specs = (
        P("img", "rep", None),
        P("img", "rep"),
        P("img", None),
        P("img", None),
        P("img", "rep", None),
        P("img", "rep"),
    )
    out_specs = (P("img", None, None), P("img"))
    return jax.shard_map(
        on_device, mesh=mesh, in_specs=in_specs, out_specs=out_specs, check_vma=False
    )
```

```python
import functools

import jax
import jax.numpy as jnp
from jax import lax
from jax.experimental import pallas as pl
from jax.experimental.pallas import tpu as pltpu
from jax.sharding import PartitionSpec as P

DESC = 128
KP = 8
GROUP = 4
QUADS = 16

dead_entry = 16384.0
cut = 1.0e6
f32 = jnp.float32
bf16 = jnp.bfloat16
i32 = jnp.int32

at_total, at_second, at_first = 64, 65, 66


def room(mib):
    return pltpu.CompilerParams(vmem_limit_bytes=mib << 20)


def vmem():
    return pl.BlockSpec(memory_space=pltpu.VMEM)


def anywhere():
    return pl.BlockSpec(memory_space=pl.ANY)


def smem():
    return pl.BlockSpec(memory_space=pltpu.SMEM)


def write_notes(rep, share, cand, query, images, live, counts, note, sources, board):
    me = lax.axis_index("rep")
    cells = 2 * share
    pairs = cand.shape[1]
    first = images[0:1, :] & 1
    second = images[1:2, :] & 1
    slot = lax.broadcasted_iota(i32, cand.shape, 0)
    rows = jnp.where(slot < live[...], second * share + (cand[...] & (share - 1)), cells)
    cell = query[...]
    quarter = lax.shift_right_logical(cell, share.bit_length() - 1)
    local = first * share + (cell & (share - 1))
    source = ((me - quarter) & (rep - 1)) * cells + local
    local = jnp.where(quarter == me, local, -1)
    ids = lax.broadcasted_iota(i32, (cells, pairs), 0)
    hits = jnp.zeros((cells, pairs), f32)
    for t in range(local.shape[0]):
        hits = hits + jnp.where(ids == local[t : t + 1, :], 1.0, 0.0)
    total = jnp.zeros((1, pairs), f32)
    for b in range(2):
        total = total + jnp.dot(
            counts[b : b + 1, :].astype(f32),
            hits[b * share : (b + 1) * share],
            preferred_element_type=f32,
        )
    board[...] = jnp.zeros_like(board)
    slots = rows.shape[0]
    spot = pl.ds(pl.multiple_of(me * slots, slots), slots)
    board[spot, 0:pairs] = rows.astype(f32) * (2.0 * KP)
    board[at_total : at_total + 1, 0:pairs] = total
    once = jnp.where(me == 0, 1, 0)
    board[at_second : at_second + 1, 0:pairs] = (second * once).astype(f32)
    board[at_first : at_first + 1, 0:pairs] = (first * once).astype(f32)
    part = sources.shape[0]
    picked = source[0:part]
    for r in range(1, rep):
        picked = jnp.where(me == r, source[r * part : (r + 1) * part], picked)
    sources[...] = jnp.zeros_like(sources)
    sources[:, 0:pairs] = picked
    note[...] = board[...].T[:pairs].astype(i32)


def pick_queries(rep, note_ref, own, one, two, three, out_ref, every, note, out, sems):
    count = own.shape[0]
    part = out.shape[1]
    block = 32
    unroll = 16
    steps = out.shape[0] // unroll
    load = pltpu.make_async_copy(note_ref, note, sems.at[steps])
    load.start()

    def fill(c, _):
        for back, source in enumerate((own, one, two, three)):
            every[pl.ds(back * count + c * block, block)] = source[pl.ds(c * block, block)]
        return 0

    lax.fori_loop(0, count // block, fill, 0)
    load.wait()

    def store(c):
        at = pl.ds(c * unroll, unroll)
        return pltpu.make_async_copy(out.at[at], out_ref.at[at], sems.at[c])

    def step(c, _):
        for k in range(unroll):
            for u in range(part):
                p = c * unroll + k
                out[p, u] = every[note[u, p]]

        @pl.when(c > 0)
        def _():
            store(c - 1).start()

        return 0

    lax.fori_loop(0, steps, step, 0)
    store(steps - 1).start()
    for c in range(steps):
        store(c).wait()


def keep_two(left, right):
    low = jnp.minimum(left[0], right[0])
    high = jnp.minimum(jnp.maximum(left[0], right[0]), jnp.minimum(left[1], right[1]))
    return low, high


def fill_tables(every, tables):
    count = every.shape[0] // len(tables)
    block = 16
    me = lax.axis_index("rep")

    def fill(c, _):
        for quarter, table in enumerate(tables):
            back = (me - quarter) & (len(tables) - 1)
            x = every[pl.ds(back * count + c * block, block)].astype(f32)
            sums = jnp.broadcast_to(jnp.sum(x * x, axis=2, keepdims=True), x.shape)
            both = jnp.concatenate([x, sums], axis=1).reshape(block * 2 * KP, DESC)
            table[pl.ds(pl.multiple_of(c * (block * 2 * KP), 2 * KP), block * 2 * KP)] = both
        return 0

    lax.fori_loop(0, count // block, fill, 0)
    for table in tables:
        end = count * 2 * KP
        table[end : end + KP] = jnp.full((KP, DESC), dead_entry, f32)
        table[end + KP : end + 2 * KP] = jnp.full((KP, DESC), dead_entry * dead_entry * DESC, f32)


def match(rep, slots, meta_ref, every, queries, out, meta, sem, *scratch):
    size = DESC // GROUP
    quads = queries.shape[0] // GROUP
    tables, norms = scratch[:rep], scratch[rep:]
    row_ids = lax.broadcasted_iota(i32, (DESC, DESC), 0)
    lane_ids = lax.broadcasted_iota(i32, (DESC, DESC), 1)
    diagonal = row_ids == lane_ids
    lanes = lax.broadcasted_iota(i32, (KP, DESC), 1)
    lane_group = lanes // size
    load = pltpu.make_async_copy(meta_ref, meta, sem)
    load.start()
    fill_tables(every, tables)
    load.wait()

    def per_group(values):
        return jnp.where(
            lane_group < 2,
            jnp.where(lane_group == 0, values[0], values[1]),
            jnp.where(lane_group == 2, values[2], values[3]),
        )

    def quad(g, norms):
        q = queries[pl.ds(g * GROUP, GROUP)].astype(f32).reshape(DESC, DESC)
        square = jnp.sum(q * q, axis=1, keepdims=True)
        spread = jnp.where(diagonal, square, 0.0).reshape(DESC // KP, KP, DESC)
        qnorm = jnp.sum(jnp.sum(spread, axis=0), axis=0, keepdims=True)
        qnorm = jnp.broadcast_to(qnorm, (KP, DESC))
        twice = q * -2.0
        blank = jnp.zeros((size, DESC), f32)
        right = jnp.concatenate(
            [
                jnp.concatenate(
                    [twice[i * size : (i + 1) * size] if i == j else blank for i in range(GROUP)],
                    axis=0,
                )
                for j in range(GROUP)
            ],
            axis=1,
        )
        columns, at = [[] for _ in range(GROUP)], 0
        for quarter, table in enumerate(tables):
            for s in range(slots):
                found = []
                for i in range(GROUP):
                    row = pl.multiple_of(meta[g * GROUP + i, quarter * slots + s], 2 * KP)
                    both = table[pl.ds(row, 2 * KP)]
                    columns[i].append(both[:KP])
                    found.append(both[KP:])
                norms[at : at + KP] = per_group(found)
                at += KP
        left = jnp.concatenate([jnp.concatenate(part, axis=0) for part in columns], axis=1)
        inner = lax.dot_general(
            left, right, (((1,), (1,)), ((), ())), preferred_element_type=f32
        )
        dist = [inner[k : k + KP] + norms[k : k + KP] for k in range(0, at, KP)]
        sides = [(dist[k], dist[k + 1]) for k in range(0, len(dist), 2)]
        sides = [(jnp.minimum(a, b), jnp.maximum(a, b)) for a, b in sides]
        while len(sides) > 1:
            sides = [keep_two(sides[k], sides[k + 1]) for k in range(0, len(sides), 2)]
        low, high = sides[0]
        for turn in (4, 2, 1):
            low, high = keep_two(
                (low, high), (pltpu.roll(low, turn, 0), pltpu.roll(high, turn, 0))
            )
        live = qnorm < cut
        best = jnp.where(live, low + qnorm, 0.0)
        runner = jnp.where(live, high + qnorm, 0.0)
        rows = [g * GROUP + i for i in range(GROUP)]
        total = per_group([meta[p, at_total].astype(f32) for p in rows])
        second = per_group([meta[p, at_second] for p in rows]).astype(f32)
        first = per_group([meta[p, at_first] for p in rows]).astype(f32)
        share = (runner - best) / ((runner + 1.0) * total)
        for i in range(GROUP):
            left, other, count, which = (
                v if at == 0 else pltpu.roll(v, at, 1)
                for v, at in (
                    (best, (DESC - size * i) % DESC),
                    (runner, (size - size * i) % DESC),
                    (total, (2 * size - size * i) % DESC),
                    (first, (2 * size - size * i) % DESC),
                )
            )
            line = jnp.where(lanes < size, left, jnp.where(lanes < 2 * size, other, count))
            line = jnp.where(lanes < 2 * size + size // 2, line, which)
            out[g * GROUP + i] = line[:rep]
        return jnp.where(second == 0.0, share, 0.0), jnp.where(second == 0.0, 0.0, share)

    def step(c, sums):
        for h in range(QUADS):
            parts = quad(c * QUADS + h, norms[h])
            sums = tuple(a + b for a, b in zip(sums, parts))
        return sums

    zero = jnp.zeros((KP, DESC), f32)
    sums = lax.fori_loop(0, quads // QUADS, step, (zero, zero))
    here = lax.axis_index("img")
    parts = [jnp.sum(part[:1], axis=1, keepdims=True) for part in sums]
    ids = lanes[:rep]
    out[here] = jnp.where(
        ids < 3 * size,
        out[here],
        jnp.where(ids < 3 * size + size // 2, parts[0], parts[1]),
    )


def finish(rep, shares, matches, scores):
    size = DESC // rep
    here = lax.axis_index("img")
    pairs = matches.shape[0]
    lane_group = lax.broadcasted_iota(i32, (pairs, DESC), 1) // size
    best = jnp.zeros((pairs, DESC), f32)
    runner = jnp.zeros((pairs, DESC), f32)
    for r in range(rep):
        part = shares[:, r, :]
        left = part if r == 0 else pltpu.roll(part, size * r, 1)
        at = (size * r - size) % DESC
        other = part if at == 0 else pltpu.roll(part, at, 1)
        best = jnp.where(lane_group == r, left, best)
        runner = jnp.where(lane_group == r, other, runner)
    matches[:, 0, :] = best
    matches[:, 1, :] = runner
    total = shares[:, 0, 2 * size : 2 * size + 1]
    score = jnp.sum((runner - best) / (runner + 1.0), axis=1, keepdims=True) / total
    at = 2 * size + size // 2
    which = shares[:, 0, at : at + 1]
    mine = shares[here]
    for b in range(2):
        own_part = jnp.sum(jnp.where(which == float(b), score, 0.0))
        at = 3 * size + b * (size // 2)
        scores[b] = own_part + jnp.sum(mine[:, at : at + 1])


def on_device(descriptors, cell_counts, pair_images, query_cells, cand_cells, cand_counts):
    img_dev, share, width = descriptors.shape
    peers = lax.axis_size("img")
    rep = lax.axis_size("rep")
    slots = cand_cells.shape[2]
    part = query_cells.shape[1] // rep
    cells = img_dev * share

    own = descriptors.reshape(img_dev, share, KP, DESC)
    own, counts = lax.optimization_barrier((own, cell_counts))
    live = lax.broadcasted_iota(i32, (img_dev, share, KP), 2) < counts[:, :, None]
    live = lax.optimization_barrier(live)
    own = jnp.where(live[:, :, :, None], own, bf16(dead_entry)).reshape(cells, KP, DESC)

    def turned(x, by):
        return lax.ppermute(x, "rep", [(r, (r + by) % rep) for r in range(rep)])

    one, two, three = (turned(own, by) for by in range(1, rep))

    note, sources = pl.pallas_call(
        functools.partial(write_notes, rep, share),
        out_shape=(
            jax.ShapeDtypeStruct((peers, DESC), i32),
            jax.ShapeDtypeStruct((part, DESC), i32),
        ),
        in_specs=[vmem()] * 5,
        out_specs=(vmem(), vmem()),
        scratch_shapes=[pltpu.VMEM((DESC, DESC), f32)],
        name="write_notes",
    )(cand_cells[:, 0, :].T, query_cells.T, pair_images.T, cand_counts.T, cell_counts)
    meta = lax.all_to_all(
        note.reshape(peers, 1, DESC), "img", split_axis=0, concat_axis=0, tiled=True
    ).reshape(peers, DESC)

    message, every = pl.pallas_call(
        functools.partial(pick_queries, rep),
        out_shape=(
            jax.ShapeDtypeStruct((peers, part, KP, DESC), bf16),
            jax.ShapeDtypeStruct((rep * cells, KP, DESC), bf16),
        ),
        in_specs=[anywhere()] + [vmem()] * 4,
        out_specs=(anywhere(), vmem()),
        scratch_shapes=[
            pltpu.SMEM((part, DESC), i32),
            pltpu.VMEM((peers, part, KP, DESC), bf16),
            pltpu.SemaphoreType.DMA((5,)),
        ],
        compiler_params=room(2),
        name="pick_queries",
    )(sources, own, one, two, three)
    queries = lax.all_to_all(
        message.reshape(peers, part * KP, DESC), "img", split_axis=0, concat_axis=0, tiled=True
    )
    meta = sum((turned(meta, by) for by in range(1, rep)), meta)

    shares = pl.pallas_call(
        functools.partial(match, rep, slots),
        out_shape=jax.ShapeDtypeStruct((peers, rep, DESC), f32),
        in_specs=[anywhere(), vmem(), vmem()],
        out_specs=vmem(),
        scratch_shapes=[pltpu.SMEM((peers, DESC), i32), pltpu.SemaphoreType.DMA]
        + [pltpu.VMEM(((cells + 1) * 2 * KP, DESC), f32)] * rep
        + [pltpu.VMEM((rep * slots * KP, DESC), f32)] * QUADS,
        compiler_params=pltpu.CompilerParams(vmem_limit_bytes=8<<20),
        name="match",
    )(meta, every, queries)
    shares = lax.all_to_all(
        shares.reshape(peers * rep, 1, DESC), ("img", "rep"), split_axis=0, concat_axis=0, tiled=True
    ).reshape(peers, rep, DESC)

    return pl.pallas_call(
        functools.partial(finish, rep),
        out_shape=(
            jax.ShapeDtypeStruct((peers, 2, DESC), f32),
            jax.ShapeDtypeStruct((img_dev,), f32),
        ),
        in_specs=[vmem()],
        out_specs=(vmem(), smem()),
        compiler_params=room(4),
        name="finish",
    )(shares)


def solution(mesh):
    in_specs = (
        P("img", "rep", None),
        P("img", "rep"),
        P("img", None),
        P("img", None),
        P("img", "rep", None),
        P("img", "rep"),
    )
    out_specs = (P("img", None, None), P("img"))
    return jax.shard_map(
        on_device, mesh=mesh, in_specs=in_specs, out_specs=out_specs, check_vma=False
    )
```

```python
import functools

import jax
import jax.numpy as jnp
from jax import lax
from jax.experimental import pallas as pl
from jax.experimental.pallas import tpu as pltpu
from jax.sharding import PartitionSpec as P

DESC = 128
KP = 8
GROUP = 4
QUADS = 16

dead_entry = 16384.0
cut = 1.0e6
f32 = jnp.float32
bf16 = jnp.bfloat16
i32 = jnp.int32

at_total, at_second, at_first, at_counts = 64, 65, 66, 72


def room(mib):
    return pltpu.CompilerParams(vmem_limit_bytes=mib << 20)


def vmem():
    return pl.BlockSpec(memory_space=pltpu.VMEM)


def anywhere():
    return pl.BlockSpec(memory_space=pl.ANY)


def smem():
    return pl.BlockSpec(memory_space=pltpu.SMEM)


def prepare(rep, share, desc, cand, query, images, live, counts, own, note, sources, board, tiles):
    me = lax.axis_index("rep")
    cells = 2 * share
    pairs = cand.shape[1]
    first = images[0:1, :] & 1
    second = images[1:2, :] & 1
    slot = lax.broadcasted_iota(i32, cand.shape, 0)
    rows = jnp.where(slot < live[...], second * share + (cand[...] & (share - 1)), cells)
    cell = query[...]
    quarter = lax.shift_right_logical(cell, share.bit_length() - 1)
    local = first * share + (cell & (share - 1))
    source = ((me - quarter) & (rep - 1)) * cells + local
    local = jnp.where(quarter == me, local, -1)
    ids = lax.broadcasted_iota(i32, (cells, pairs), 0)
    hits = jnp.zeros((cells, pairs), f32)
    for t in range(local.shape[0]):
        hits = hits + jnp.where(ids == local[t : t + 1, :], 1.0, 0.0)
    total = jnp.zeros((1, pairs), f32)
    for b in range(2):
        total = total + jnp.dot(
            counts[b : b + 1, :].astype(f32),
            hits[b * share : (b + 1) * share],
            preferred_element_type=f32,
        )
    board[...] = jnp.zeros_like(board)
    slots = rows.shape[0]
    spot = pl.ds(pl.multiple_of(me * slots, slots), slots)
    board[spot, 0:pairs] = rows.astype(f32) * (2.0 * KP)
    board[at_total : at_total + 1, 0:pairs] = total
    once = jnp.where(me == 0, 1, 0)
    board[at_second : at_second + 1, 0:pairs] = (second * once).astype(f32)
    board[at_first : at_first + 1, 0:pairs] = (first * once).astype(f32)
    part = sources.shape[0]
    picked = source[0:part]
    for r in range(1, rep):
        picked = jnp.where(me == r, source[r * part : (r + 1) * part], picked)
    sources[...] = jnp.zeros_like(sources)
    sources[:, 0:pairs] = picked
    board[at_counts : at_counts + 2, 0:pairs] = counts[...].astype(f32)
    turned = board[...].T[:pairs]
    note[...] = turned.astype(i32)
    for b in range(2):
        column = turned[:, at_counts + b : at_counts + b + 1]
        for s in range(KP):
            x = desc[b, :, s * DESC : (s + 1) * DESC].astype(f32)
            x = jnp.where(column > float(s), x, dead_entry)
            tiles[pl.ds(b * share * KP + s, share, stride=KP), :] = x
    own[...] = tiles[...].reshape(cells, KP, DESC).astype(bf16)


def pick_queries(rep, note_ref, own, one, two, three, out_ref, every, note, out, sems):
    count = own.shape[0]
    part = out.shape[1]
    block = 32
    unroll = 16
    steps = out.shape[0] // unroll
    load = pltpu.make_async_copy(note_ref, note, sems.at[steps])
    load.start()

    def fill(c, _):
        for back, source in enumerate((own, one, two, three)):
            every[pl.ds(back * count + c * block, block)] = source[pl.ds(c * block, block)]
        return 0

    lax.fori_loop(0, count // block, fill, 0)
    load.wait()

    def store(c):
        at = pl.ds(c * unroll, unroll)
        return pltpu.make_async_copy(out.at[at], out_ref.at[at], sems.at[c])

    def step(c, _):
        for k in range(unroll):
            for u in range(part):
                p = c * unroll + k
                out[p, u] = every[note[u, p]]

        @pl.when(c > 0)
        def _():
            store(c - 1).start()

        return 0

    lax.fori_loop(0, steps, step, 0)
    store(steps - 1).start()
    for c in range(steps):
        store(c).wait()


def keep_two(left, right):
    low = jnp.minimum(left[0], right[0])
    high = jnp.minimum(jnp.maximum(left[0], right[0]), jnp.minimum(left[1], right[1]))
    return low, high


def fill_tables(every, tables):
    count = every.shape[0] // len(tables)
    block = 16
    me = lax.axis_index("rep")

    def fill(c, _):
        for quarter, table in enumerate(tables):
            back = (me - quarter) & (len(tables) - 1)
            x = every[pl.ds(back * count + c * block, block)].astype(f32)
            sums = jnp.broadcast_to(jnp.sum(x * x, axis=2, keepdims=True), x.shape)
            both = jnp.concatenate([x, sums], axis=1).reshape(block * 2 * KP, DESC)
            table[pl.ds(pl.multiple_of(c * (block * 2 * KP), 2 * KP), block * 2 * KP)] = both
        return 0

    lax.fori_loop(0, count // block, fill, 0)
    for table in tables:
        end = count * 2 * KP
        table[end : end + KP] = jnp.full((KP, DESC), dead_entry, f32)
        table[end + KP : end + 2 * KP] = jnp.full((KP, DESC), dead_entry * dead_entry * DESC, f32)


def match(rep, slots, meta_ref, every, queries, out, meta, sem, *scratch):
    size = DESC // GROUP
    quads = queries.shape[0] // GROUP
    tables, norms = scratch[:rep], scratch[rep:]
    row_ids = lax.broadcasted_iota(i32, (DESC, DESC), 0)
    lane_ids = lax.broadcasted_iota(i32, (DESC, DESC), 1)
    diagonal = row_ids == lane_ids
    lanes = lax.broadcasted_iota(i32, (KP, DESC), 1)
    lane_group = lanes // size
    load = pltpu.make_async_copy(meta_ref, meta, sem)
    load.start()
    fill_tables(every, tables)
    load.wait()

    def per_group(values):
        return jnp.where(
            lane_group < 2,
            jnp.where(lane_group == 0, values[0], values[1]),
            jnp.where(lane_group == 2, values[2], values[3]),
        )

    def quad(g, norms):
        q = queries[pl.ds(g * GROUP, GROUP)].astype(f32).reshape(DESC, DESC)
        square = jnp.sum(q * q, axis=1, keepdims=True)
        spread = jnp.where(diagonal, square, 0.0).reshape(DESC // KP, KP, DESC)
        qnorm = jnp.sum(jnp.sum(spread, axis=0), axis=0, keepdims=True)
        qnorm = jnp.broadcast_to(qnorm, (KP, DESC))
        twice = q * -2.0
        blank = jnp.zeros((size, DESC), f32)
        right = jnp.concatenate(
            [
                jnp.concatenate(
                    [twice[i * size : (i + 1) * size] if i == j else blank for i in range(GROUP)],
                    axis=0,
                )
                for j in range(GROUP)
            ],
            axis=1,
        )
        columns, at = [[] for _ in range(GROUP)], 0
        for quarter, table in enumerate(tables):
            for s in range(slots):
                found = []
                for i in range(GROUP):
                    row = pl.multiple_of(meta[g * GROUP + i, quarter * slots + s], 2 * KP)
                    both = table[pl.ds(row, 2 * KP)]
                    columns[i].append(both[:KP])
                    found.append(both[KP:])
                norms[at : at + KP] = per_group(found)
                at += KP
        left = jnp.concatenate([jnp.concatenate(part, axis=0) for part in columns], axis=1)
        inner = lax.dot_general(
            left, right, (((1,), (1,)), ((), ())), preferred_element_type=f32
        )
        dist = [inner[k : k + KP] + norms[k : k + KP] for k in range(0, at, KP)]
        sides = [(dist[k], dist[k + 1]) for k in range(0, len(dist), 2)]
        sides = [(jnp.minimum(a, b), jnp.maximum(a, b)) for a, b in sides]
        while len(sides) > 1:
            sides = [keep_two(sides[k], sides[k + 1]) for k in range(0, len(sides), 2)]
        low, high = sides[0]
        for turn in (4, 2, 1):
            low, high = keep_two(
                (low, high), (pltpu.roll(low, turn, 0), pltpu.roll(high, turn, 0))
            )
        live = qnorm < cut
        best = jnp.where(live, low + qnorm, 0.0)
        runner = jnp.where(live, high + qnorm, 0.0)
        rows = [g * GROUP + i for i in range(GROUP)]
        total = per_group([meta[p, at_total].astype(f32) for p in rows])
        second = per_group([meta[p, at_second] for p in rows]).astype(f32)
        first = per_group([meta[p, at_first] for p in rows]).astype(f32)
        share = (runner - best) / ((runner + 1.0) * total)
        for i in range(GROUP):
            left, other, count, which = (
                v if at == 0 else pltpu.roll(v, at, 1)
                for v, at in (
                    (best, (DESC - size * i) % DESC),
                    (runner, (size - size * i) % DESC),
                    (total, (2 * size - size * i) % DESC),
                    (first, (2 * size - size * i) % DESC),
                )
            )
            line = jnp.where(lanes < size, left, jnp.where(lanes < 2 * size, other, count))
            line = jnp.where(lanes < 2 * size + size // 2, line, which)
            out[g * GROUP + i] = line[:rep]
        return jnp.where(second == 0.0, share, 0.0), jnp.where(second == 0.0, 0.0, share)

    def step(c, sums):
        for h in range(QUADS):
            parts = quad(c * QUADS + h, norms[h])
            sums = tuple(a + b for a, b in zip(sums, parts))
        return sums

    zero = jnp.zeros((KP, DESC), f32)
    sums = lax.fori_loop(0, quads // QUADS, step, (zero, zero))
    here = lax.axis_index("img")
    parts = [jnp.sum(part[:1], axis=1, keepdims=True) for part in sums]
    ids = lanes[:rep]
    out[here] = jnp.where(
        ids < 3 * size,
        out[here],
        jnp.where(ids < 3 * size + size // 2, parts[0], parts[1]),
    )


def finish(rep, shares, matches, scores):
    size = DESC // rep
    here = lax.axis_index("img")
    pairs = matches.shape[0]
    lane_group = lax.broadcasted_iota(i32, (pairs, DESC), 1) // size
    best = jnp.zeros((pairs, DESC), f32)
    runner = jnp.zeros((pairs, DESC), f32)
    for r in range(rep):
        part = shares[:, r, :]
        left = part if r == 0 else pltpu.roll(part, size * r, 1)
        at = (size * r - size) % DESC
        other = part if at == 0 else pltpu.roll(part, at, 1)
        best = jnp.where(lane_group == r, left, best)
        runner = jnp.where(lane_group == r, other, runner)
    matches[:, 0, :] = best
    matches[:, 1, :] = runner
    total = shares[:, 0, 2 * size : 2 * size + 1]
    score = jnp.sum((runner - best) / (runner + 1.0), axis=1, keepdims=True) / total
    at = 2 * size + size // 2
    which = shares[:, 0, at : at + 1]
    mine = shares[here]
    for b in range(2):
        own_part = jnp.sum(jnp.where(which == float(b), score, 0.0))
        at = 3 * size + b * (size // 2)
        scores[b] = own_part + jnp.sum(mine[:, at : at + 1])


def on_device(descriptors, cell_counts, pair_images, query_cells, cand_cells, cand_counts):
    img_dev, share, width = descriptors.shape
    peers = lax.axis_size("img")
    rep = lax.axis_size("rep")
    slots = cand_cells.shape[2]
    part = query_cells.shape[1] // rep
    cells = img_dev * share

    def turned(x, by):
        return lax.ppermute(x, "rep", [(r, (r + by) % rep) for r in range(rep)])

    own, note, sources = pl.pallas_call(
        functools.partial(prepare, rep, share),
        out_shape=(
            jax.ShapeDtypeStruct((cells, KP, DESC), bf16),
            jax.ShapeDtypeStruct((peers, DESC), i32),
            jax.ShapeDtypeStruct((part, DESC), i32),
        ),
        in_specs=[vmem()] * 6,
        out_specs=(vmem(), vmem(), vmem()),
        scratch_shapes=[pltpu.VMEM((DESC, DESC), f32), pltpu.VMEM((cells * KP, DESC), f32)],
        name="prepare",
    )(
        descriptors,
        cand_cells[:, 0, :].T,
        query_cells.T,
        pair_images.T,
        cand_counts.T,
        cell_counts,
    )
    one, two, three = (turned(own, by) for by in range(1, rep))

    meta = lax.all_to_all(
        note.reshape(peers, 1, DESC), "img", split_axis=0, concat_axis=0, tiled=True
    ).reshape(peers, DESC)

    message, every = pl.pallas_call(
        functools.partial(pick_queries, rep),
        out_shape=(
            jax.ShapeDtypeStruct((peers, part, KP, DESC), bf16),
            jax.ShapeDtypeStruct((rep * cells, KP, DESC), bf16),
        ),
        in_specs=[anywhere()] + [vmem()] * 4,
        out_specs=(anywhere(), vmem()),
        scratch_shapes=[
            pltpu.SMEM((part, DESC), i32),
            pltpu.VMEM((peers, part, KP, DESC), bf16),
            pltpu.SemaphoreType.DMA((5,)),
        ],
        compiler_params=room(2),
        name="pick_queries",
    )(sources, own, one, two, three)
    queries = lax.all_to_all(
        message.reshape(peers, part * KP, DESC), "img", split_axis=0, concat_axis=0, tiled=True
    )
    meta = sum((turned(meta, by) for by in range(1, rep)), meta)

    shares = pl.pallas_call(
        functools.partial(match, rep, slots),
        out_shape=jax.ShapeDtypeStruct((peers, rep, DESC), f32),
        in_specs=[anywhere(), vmem(), vmem()],
        out_specs=vmem(),
        scratch_shapes=[pltpu.SMEM((peers, DESC), i32), pltpu.SemaphoreType.DMA]
        + [pltpu.VMEM(((cells + 1) * 2 * KP, DESC), f32)] * rep
        + [pltpu.VMEM((rep * slots * KP, DESC), f32)] * QUADS,
        compiler_params=pltpu.CompilerParams(vmem_limit_bytes=8<<20),
        name="match",
    )(meta, every, queries)
    shares = lax.all_to_all(
        shares.reshape(peers * rep, 1, DESC), ("img", "rep"), split_axis=0, concat_axis=0, tiled=True
    ).reshape(peers, rep, DESC)

    return pl.pallas_call(
        functools.partial(finish, rep),
        out_shape=(
            jax.ShapeDtypeStruct((peers, 2, DESC), f32),
            jax.ShapeDtypeStruct((img_dev,), f32),
        ),
        in_specs=[vmem()],
        out_specs=(vmem(), smem()),
        compiler_params=room(4),
        name="finish",
    )(shares)


def solution(mesh):
    in_specs = (
        P("img", "rep", None),
        P("img", "rep"),
        P("img", None),
        P("img", None),
        P("img", "rep", None),
        P("img", "rep"),
    )
    out_specs = (P("img", None, None), P("img"))
    return jax.shard_map(
        on_device, mesh=mesh, in_specs=in_specs, out_specs=out_specs, check_vma=False
    )
```

```python
import functools

import jax
import jax.numpy as jnp
from jax import lax
from jax.experimental import pallas as pl
from jax.experimental.pallas import tpu as pltpu
from jax.sharding import PartitionSpec as P

DESC = 128
KP = 8
GROUP = 4
QUADS = 16

dead_entry = 16384.0
cut = 1.0e6
f32 = jnp.float32
bf16 = jnp.bfloat16
i32 = jnp.int32

at_total, at_second, at_first, at_counts = 64, 65, 66, 72


def room(mib):
    return pltpu.CompilerParams(vmem_limit_bytes=mib << 20)


def vmem():
    return pl.BlockSpec(memory_space=pltpu.VMEM)


def anywhere():
    return pl.BlockSpec(memory_space=pl.ANY)


def smem():
    return pl.BlockSpec(memory_space=pltpu.SMEM)


def prepare(rep, share, desc, cand, query, images, live, counts, own, note, sources, board, tiles):
    me = lax.axis_index("rep")
    cells = 2 * share
    pairs = cand.shape[1]
    first = images[0:1, :] & 1
    second = images[1:2, :] & 1
    slot = lax.broadcasted_iota(i32, cand.shape, 0)
    rows = jnp.where(slot < live[...], second * share + (cand[...] & (share - 1)), cells)
    cell = query[...]
    quarter = lax.shift_right_logical(cell, share.bit_length() - 1)
    local = first * share + (cell & (share - 1))
    source = ((me - quarter) & (rep - 1)) * cells + local
    local = jnp.where(quarter == me, local, -1)
    ids = lax.broadcasted_iota(i32, (cells, pairs), 0)
    hits = jnp.zeros((cells, pairs), f32)
    for t in range(local.shape[0]):
        hits = hits + jnp.where(ids == local[t : t + 1, :], 1.0, 0.0)
    total = jnp.zeros((1, pairs), f32)
    for b in range(2):
        total = total + jnp.dot(
            counts[b : b + 1, :].astype(f32),
            hits[b * share : (b + 1) * share],
            preferred_element_type=f32,
        )
    board[...] = jnp.zeros_like(board)
    slots = rows.shape[0]
    spot = pl.ds(pl.multiple_of(me * slots, slots), slots)
    board[spot, 0:pairs] = rows.astype(f32) * (2.0 * KP)
    board[at_total : at_total + 1, 0:pairs] = total
    once = jnp.where(me == 0, 1, 0)
    board[at_second : at_second + 1, 0:pairs] = (second * once).astype(f32)
    board[at_first : at_first + 1, 0:pairs] = (first * once).astype(f32)
    part = sources.shape[0]
    picked = source[0:part]
    for r in range(1, rep):
        picked = jnp.where(me == r, source[r * part : (r + 1) * part], picked)
    sources[...] = jnp.zeros_like(sources)
    sources[:, 0:pairs] = picked
    board[at_counts : at_counts + 2, 0:pairs] = counts[...].astype(f32)
    turned = board[...].T[:pairs]
    note[...] = turned.astype(i32)
    for b in range(2):
        column = turned[:, at_counts + b : at_counts + b + 1]
        for s in range(KP):
            x = desc[b, :, s * DESC : (s + 1) * DESC].astype(f32)
            x = jnp.where(column > float(s), x, dead_entry)
            tiles[pl.ds(b * share * KP + s, share, stride=KP), :] = x
    own[...] = tiles[...].reshape(cells, KP, DESC).astype(bf16)


def pick_queries(rep, note_ref, own, one, two, three, out_ref, every, note, out, sems):
    count = own.shape[0]
    part = out.shape[1]
    block = 32
    unroll = 16
    steps = out.shape[0] // unroll
    load = pltpu.make_async_copy(note_ref, note, sems.at[steps])
    load.start()

    def fill(c, _):
        for back, source in enumerate((own, one, two, three)):
            every[pl.ds(back * count + c * block, block)] = source[pl.ds(c * block, block)]
        return 0

    lax.fori_loop(0, count // block, fill, 0)
    load.wait()

    def store(c):
        at = pl.ds(c * unroll, unroll)
        return pltpu.make_async_copy(out.at[at], out_ref.at[at], sems.at[c])

    def step(c):
        for k in range(unroll):
            for u in range(part):
                p = c * unroll + k
                out[p, u] = every[note[u, p]]

        if c > 0:
            store(c - 1).start()

    for c in range(steps):
        step(c)
    store(steps - 1).start()
    for c in range(steps):
        store(c).wait()


def keep_two(left, right):
    low = jnp.minimum(left[0], right[0])
    high = jnp.minimum(jnp.maximum(left[0], right[0]), jnp.minimum(left[1], right[1]))
    return low, high


def fill_tables(every, tables):
    count = every.shape[0] // len(tables)
    block = 16
    me = lax.axis_index("rep")

    def fill(c, _):
        for quarter, table in enumerate(tables):
            back = (me - quarter) & (len(tables) - 1)
            x = every[pl.ds(back * count + c * block, block)].astype(f32)
            sums = jnp.broadcast_to(jnp.sum(x * x, axis=2, keepdims=True), x.shape)
            both = jnp.concatenate([x, sums], axis=1).reshape(block * 2 * KP, DESC)
            table[pl.ds(pl.multiple_of(c * (block * 2 * KP), 2 * KP), block * 2 * KP)] = both
        return 0

    lax.fori_loop(0, count // block, fill, 0)
    for table in tables:
        end = count * 2 * KP
        table[end : end + KP] = jnp.full((KP, DESC), dead_entry, f32)
        table[end + KP : end + 2 * KP] = jnp.full((KP, DESC), dead_entry * dead_entry * DESC, f32)


def match(rep, slots, meta_ref, every, queries, out, meta, sem, *scratch):
    size = DESC // GROUP
    quads = queries.shape[0] // GROUP
    tables, norms = scratch[:rep], scratch[rep:]
    row_ids = lax.broadcasted_iota(i32, (DESC, DESC), 0)
    lane_ids = lax.broadcasted_iota(i32, (DESC, DESC), 1)
    diagonal = row_ids == lane_ids
    lanes = lax.broadcasted_iota(i32, (KP, DESC), 1)
    lane_group = lanes // size
    load = pltpu.make_async_copy(meta_ref, meta, sem)
    load.start()
    fill_tables(every, tables)
    load.wait()

    def per_group(values):
        return jnp.where(
            lane_group < 2,
            jnp.where(lane_group == 0, values[0], values[1]),
            jnp.where(lane_group == 2, values[2], values[3]),
        )

    def quad(g, norms):
        q = queries[pl.ds(g * GROUP, GROUP)].astype(f32).reshape(DESC, DESC)
        square = jnp.sum(q * q, axis=1, keepdims=True)
        spread = jnp.where(diagonal, square, 0.0).reshape(DESC // KP, KP, DESC)
        qnorm = jnp.sum(jnp.sum(spread, axis=0), axis=0, keepdims=True)
        qnorm = jnp.broadcast_to(qnorm, (KP, DESC))
        twice = q * -2.0
        blank = jnp.zeros((size, DESC), f32)
        right = jnp.concatenate(
            [
                jnp.concatenate(
                    [twice[i * size : (i + 1) * size] if i == j else blank for i in range(GROUP)],
                    axis=0,
                )
                for j in range(GROUP)
            ],
            axis=1,
        )
        columns, at = [[] for _ in range(GROUP)], 0
        for quarter, table in enumerate(tables):
            for s in range(slots):
                found = []
                for i in range(GROUP):
                    row = pl.multiple_of(meta[g * GROUP + i, quarter * slots + s], 2 * KP)
                    both = table[pl.ds(row, 2 * KP)]
                    columns[i].append(both[:KP])
                    found.append(both[KP:])
                norms[at : at + KP] = per_group(found)
                at += KP
        left = jnp.concatenate([jnp.concatenate(part, axis=0) for part in columns], axis=1)
        inner = lax.dot_general(
            left, right, (((1,), (1,)), ((), ())), preferred_element_type=f32
        )
        dist = [inner[k : k + KP] + norms[k : k + KP] for k in range(0, at, KP)]
        sides = [(dist[k], dist[k + 1]) for k in range(0, len(dist), 2)]
        sides = [(jnp.minimum(a, b), jnp.maximum(a, b)) for a, b in sides]
        while len(sides) > 1:
            sides = [keep_two(sides[k], sides[k + 1]) for k in range(0, len(sides), 2)]
        low, high = sides[0]
        for turn in (4, 2, 1):
            low, high = keep_two(
                (low, high), (pltpu.roll(low, turn, 0), pltpu.roll(high, turn, 0))
            )
        live = qnorm < cut
        best = jnp.where(live, low + qnorm, 0.0)
        runner = jnp.where(live, high + qnorm, 0.0)
        rows = [g * GROUP + i for i in range(GROUP)]
        total = per_group([meta[p, at_total].astype(f32) for p in rows])
        second = per_group([meta[p, at_second] for p in rows]).astype(f32)
        first = per_group([meta[p, at_first] for p in rows]).astype(f32)
        share = (runner - best) / ((runner + 1.0) * total)
        for i in range(GROUP):
            left, other, count, which = (
                v if at == 0 else pltpu.roll(v, at, 1)
                for v, at in (
                    (best, (DESC - size * i) % DESC),
                    (runner, (size - size * i) % DESC),
                    (total, (2 * size - size * i) % DESC),
                    (first, (2 * size - size * i) % DESC),
                )
            )
            line = jnp.where(lanes < size, left, jnp.where(lanes < 2 * size, other, count))
            line = jnp.where(lanes < 2 * size + size // 2, line, which)
            out[g * GROUP + i] = line[:rep]
        return jnp.where(second == 0.0, share, 0.0), jnp.where(second == 0.0, 0.0, share)

    def step(c, sums):
        for h in range(QUADS):
            parts = quad(c * QUADS + h, norms[h])
            sums = tuple(a + b for a, b in zip(sums, parts))
        return sums

    zero = jnp.zeros((KP, DESC), f32)
    sums = lax.fori_loop(0, quads // QUADS, step, (zero, zero))
    here = lax.axis_index("img")
    parts = [jnp.sum(part[:1], axis=1, keepdims=True) for part in sums]
    ids = lanes[:rep]
    out[here] = jnp.where(
        ids < 3 * size,
        out[here],
        jnp.where(ids < 3 * size + size // 2, parts[0], parts[1]),
    )


def finish(rep, shares, matches, scores):
    size = DESC // rep
    here = lax.axis_index("img")
    pairs = matches.shape[0]
    lane_group = lax.broadcasted_iota(i32, (pairs, DESC), 1) // size
    best = jnp.zeros((pairs, DESC), f32)
    runner = jnp.zeros((pairs, DESC), f32)
    for r in range(rep):
        part = shares[:, r, :]
        left = part if r == 0 else pltpu.roll(part, size * r, 1)
        at = (size * r - size) % DESC
        other = part if at == 0 else pltpu.roll(part, at, 1)
        best = jnp.where(lane_group == r, left, best)
        runner = jnp.where(lane_group == r, other, runner)
    matches[:, 0, :] = best
    matches[:, 1, :] = runner
    total = shares[:, 0, 2 * size : 2 * size + 1]
    score = jnp.sum((runner - best) / (runner + 1.0), axis=1, keepdims=True) / total
    at = 2 * size + size // 2
    which = shares[:, 0, at : at + 1]
    mine = shares[here]
    for b in range(2):
        own_part = jnp.sum(jnp.where(which == float(b), score, 0.0))
        at = 3 * size + b * (size // 2)
        scores[b] = own_part + jnp.sum(mine[:, at : at + 1])


def on_device(descriptors, cell_counts, pair_images, query_cells, cand_cells, cand_counts):
    img_dev, share, width = descriptors.shape
    peers = lax.axis_size("img")
    rep = lax.axis_size("rep")
    slots = cand_cells.shape[2]
    part = query_cells.shape[1] // rep
    cells = img_dev * share

    def turned(x, by):
        return lax.ppermute(x, "rep", [(r, (r + by) % rep) for r in range(rep)])

    own, note, sources = pl.pallas_call(
        functools.partial(prepare, rep, share),
        out_shape=(
            jax.ShapeDtypeStruct((cells, KP, DESC), bf16),
            jax.ShapeDtypeStruct((peers, DESC), i32),
            jax.ShapeDtypeStruct((part, DESC), i32),
        ),
        in_specs=[vmem()] * 6,
        out_specs=(vmem(), vmem(), vmem()),
        scratch_shapes=[pltpu.VMEM((DESC, DESC), f32), pltpu.VMEM((cells * KP, DESC), f32)],
        name="prepare",
    )(
        descriptors,
        cand_cells[:, 0, :].T,
        query_cells.T,
        pair_images.T,
        cand_counts.T,
        cell_counts,
    )
    one, two, three = (turned(own, by) for by in range(1, rep))

    meta = lax.all_to_all(
        note.reshape(peers, 1, DESC), "img", split_axis=0, concat_axis=0, tiled=True
    ).reshape(peers, DESC)

    message, every = pl.pallas_call(
        functools.partial(pick_queries, rep),
        out_shape=(
            jax.ShapeDtypeStruct((peers, part, KP, DESC), bf16),
            jax.ShapeDtypeStruct((rep * cells, KP, DESC), bf16),
        ),
        in_specs=[anywhere()] + [vmem()] * 4,
        out_specs=(anywhere(), vmem()),
        scratch_shapes=[
            pltpu.SMEM((part, DESC), i32),
            pltpu.VMEM((peers, part, KP, DESC), bf16),
            pltpu.SemaphoreType.DMA((5,)),
        ],
        compiler_params=room(2),
        name="pick_queries",
    )(sources, jnp.maximum(own, bf16(-dead_entry)), one, two, three)
    queries = lax.all_to_all(
        message.reshape(peers, part * KP, DESC), "img", split_axis=0, concat_axis=0, tiled=True
    )
    meta = sum((turned(meta, by) for by in range(1, rep)), meta)

    shares = pl.pallas_call(
        functools.partial(match, rep, slots),
        out_shape=jax.ShapeDtypeStruct((peers, rep, DESC), f32),
        in_specs=[anywhere(), vmem(), vmem()],
        out_specs=vmem(),
        scratch_shapes=[pltpu.SMEM((peers, DESC), i32), pltpu.SemaphoreType.DMA]
        + [pltpu.VMEM(((cells + 1) * 2 * KP, DESC), f32)] * rep
        + [pltpu.VMEM((rep * slots * KP, DESC), f32)] * QUADS,
        compiler_params=pltpu.CompilerParams(vmem_limit_bytes=8<<20),
        name="match",
    )(meta, every, queries)
    shares = lax.all_to_all(
        shares.reshape(peers * rep, 1, DESC), ("img", "rep"), split_axis=0, concat_axis=0, tiled=True
    ).reshape(peers, rep, DESC)

    return pl.pallas_call(
        functools.partial(finish, rep),
        out_shape=(
            jax.ShapeDtypeStruct((peers, 2, DESC), f32),
            jax.ShapeDtypeStruct((img_dev,), f32),
        ),
        in_specs=[vmem()],
        out_specs=(vmem(), smem()),
        compiler_params=room(4),
        name="finish",
    )(shares)


def solution(mesh):
    in_specs = (
        P("img", "rep", None),
        P("img", "rep"),
        P("img", None),
        P("img", None),
        P("img", "rep", None),
        P("img", "rep"),
    )
    out_specs = (P("img", None, None), P("img"))
    return jax.shard_map(
        on_device, mesh=mesh, in_specs=in_specs, out_specs=out_specs, check_vma=False
    )
```
